32 devices in a mesh: fsdp: 8 (over z, y), dom: 4 (over x, core).
Axes of the slice: x: 2, y: 2, z: 4, core: 2. Of those that a mesh axis runs over, the one named last changes fastest.
Arguments:
- hidden_states: bfloat16 [256, 128, 768], P(('fsdp', 'dom')), may hold values from -40 to 40
- title_tokens: int32 [256, 128], P(('fsdp', 'dom')), may hold values from 0 to 30521, as said below
- query_key_value: bfloat16 [768, 2304], P('fsdp'), may hold values from -0.5 to 2.5
- output_weight: bfloat16 [768, 768], P('fsdp'), may hold values from -0.21875 to 0.21875
- up_weight: bfloat16 [768, 3072], P('fsdp'), may hold values from -0.21875 to 0.21875
- down_weight: bfloat16 [3072, 768], P('fsdp'), may hold values from -0.109375 to 0.109375
- attention_gain: float32 [768], replicated, may hold values from 0.25 to 1.75
- feedforward_gain: float32 [768], replicated, may hold values from 0.25 to 1.75
- encoded: bfloat16 [16384, 768], P(('fsdp', 'dom')), may hold values from -6 to 6
- send_rows: int32 [32, 32, 48], P(('fsdp', 'dom')), may hold values from 0 to 511
- send_count: int32 [32, 32], P(('fsdp', 'dom')), may hold values from 6 to 48, as said below
- arrival_nodes: int32 [32, 32, 48], P(('fsdp', 'dom')), may hold values from 0 to 511
- sage_weight: bfloat16 [2, 768, 1024], P(None, 'fsdp'), may hold values from -0.21875 to 0.21875
- node_gain: float32 [1024], replicated, may hold values from 0.25 to 1.75
Outputs:
- title_vectors: bfloat16 [256, 768], P(('fsdp', 'dom'))
- node_output: bfloat16 [16384, 1024], P(('fsdp', 'dom'))
The draws below stay inside these ranges and needn't reach their ends.
Inputs may be any that keep to these rules, and one draw needn't show every extreme that they name: `title_tokens`: in each title the nonzero ids come first and zeros fill the rest; at least 16 ids of every title are nonzero. `send_count`: in every draw some device receives exactly 48 valid slots from every device.
All inputs are finite; a program needn't handle non-finite values.
Results may differ from the reference program's by a relative error of at most 0.0056.
Values may be sent and summed in bfloat16 or wider, within the bound.
A program may use at most 192 MiB of HBM per device.

```python
import math
import jax
import jax.numpy as jnp
from jax import lax

D = 768
HEADS = 12
HEAD_DIM = 64
FF = 3072
VOCAB = 30522
H = 1024
SEQ = 128
CAP = 48
TITLES_DEV = 8
NODES_DEV = 512
TITLES = 256
NODES = 16384
DEVICES = 32


def draw_hidden_states(key, part):
    streams = jax.random.split(key, 3)
    shape = (TITLES, SEQ, D)
    column_scale = jnp.exp(jax.random.uniform(streams[1], (D,), jnp.float32, math.log(0.3), math.log(3.0)))
    base = jax.random.normal(streams[0], shape, jnp.float32)
    row_scale = jnp.exp(jax.random.uniform(streams[2], (TITLES, SEQ, 1), jnp.float32, math.log(0.5), math.log(2.0)))
    values = base * row_scale * column_scale
    return jnp.clip(values, -40.0, 40.0).astype(jnp.bfloat16)


def draw_title_tokens(key, part):
    streams = jax.random.split(key, 2)
    lengths = jax.random.randint(streams[0], (TITLES, 1), SEQ // 8, SEQ + 1)
    idents = jax.random.randint(streams[1], (TITLES, SEQ), 1, VOCAB)
    position = jnp.arange(SEQ)[None, :]
    return jnp.where(position < lengths, idents, 0).astype(jnp.int32)


def draw_query_key_value(key, part):
    values = jnp.clip(jax.random.normal(key, (D, 3 * D), jnp.float32) * (1.0 / math.sqrt(D)), -0.5, 0.5)
    return values.astype(jnp.bfloat16)


def draw_send_count(key, part):
    streams = jax.random.split(key, 2)
    base = jax.random.randint(streams[0], (DEVICES, DEVICES), CAP // 8, CAP // 2 + 1)
    hottest = jax.random.randint(streams[1], (), 0, DEVICES)
    columns = jnp.arange(DEVICES)
    return jnp.where(columns[None, :] == hottest, CAP, base).astype(jnp.int32)


def draw_arrival_nodes(key, part):
    streams = jax.random.split(key, 3)
    shape = (DEVICES, DEVICES, CAP)
    first = jax.random.randint(streams[0], shape, 0, NODES_DEV)
    second = jax.random.randint(streams[1], shape, 0, NODES_DEV)
    lower = jnp.minimum(first, second).reshape(DEVICES, DEVICES * CAP)
    orders = jax.vmap(lambda stream: jax.random.permutation(stream, NODES_DEV))(jax.random.split(streams[2], DEVICES))
    picked = jnp.take_along_axis(orders.astype(jnp.int32), lower.astype(jnp.int32), axis=1)
    return picked.reshape(shape).astype(jnp.int32)


def place_ends(entries, own_key, least, top_value):
    index_at = [jax.random.randint(jax.random.fold_in(own_key, axis), (), 0, length) for axis, length in enumerate(entries.shape)]
    main_axis = entries.shape.index(max(entries.shape))
    beside = index_at[:main_axis] + [(index_at[main_axis] + 1) % entries.shape[main_axis]] + index_at[main_axis + 1:]
    return entries.at[tuple(index_at)].set(least).at[tuple(beside)].set(top_value)


def block_levels(rng, dims, pieces, least, largest):
    level = 1.0
    for axis_at, parts in pieces:
        heights = jax.random.uniform(jax.random.fold_in(jax.random.fold_in(rng, 6), axis_at), (parts,), jnp.float32, least / len(pieces), largest / len(pieces))
        level = level * jnp.repeat(jnp.exp(heights), dims[axis_at] // parts).reshape((-1,) + (1,) * (len(dims) - 1 - axis_at))
    return level


def gaussian(own_key, dims, scale, most, cuts=(), kind=jnp.bfloat16):
    level = block_levels(own_key, dims, cuts, -0.22, 0.18) if cuts else 1.0
    entries = jax.random.normal(own_key, dims, jnp.float32) * scale * level
    return jnp.minimum(jnp.maximum(entries, -most), most).astype(kind)


def setup_inputs(seed: int = 0) -> dict:
    key_of = jax.random.split(jax.random.key(seed), 15)
    hidden_states = draw_hidden_states(jax.random.fold_in(key_of[14], 71), 0)
    title_tokens = draw_title_tokens(jax.random.fold_in(key_of[14], 71), 0)
    query_key_value = draw_query_key_value(jax.random.fold_in(key_of[14], 71), 0)
    output_weight = gaussian(key_of[3], (D, D), D ** -0.5, 0.21875, ((0, 8),))
    up_weight = gaussian(key_of[4], (D, FF), D ** -0.5, 0.21875, ((0, 8),))
    down_weight = gaussian(key_of[5], (FF, D), FF ** -0.5, 0.109375, ((0, 8),))
    attention_gain = jnp.clip(1.0 + 0.15 * jax.random.normal(key_of[6], (D,), jnp.float32), 0.25, 1.75)
    feedforward_gain = jnp.clip(1.0 + 0.15 * jax.random.normal(key_of[7], (D,), jnp.float32), 0.25, 1.75)
    encoded = gaussian(key_of[8], (NODES, D), 1.0, 6.0, ((0, 32),))
    send_rows = place_ends(jax.random.randint(key_of[9], (DEVICES, DEVICES, CAP), 0, NODES_DEV), jax.random.fold_in(key_of[9], 1), 0, NODES_DEV - 1).astype(jnp.int32)
    send_count = draw_send_count(jax.random.fold_in(key_of[14], 71), 0)
    arrival_nodes = draw_arrival_nodes(jax.random.fold_in(key_of[14], 71), 0)
    sage_weight = gaussian(key_of[12], (2, D, H), D ** -0.5, 0.21875, ((1, 8),))
    node_gain = jnp.clip(1.0 + 0.15 * jax.random.normal(key_of[13], (H,), jnp.float32), 0.25, 1.75)
    return dict(hidden_states=hidden_states, title_tokens=title_tokens, query_key_value=query_key_value, output_weight=output_weight, up_weight=up_weight, down_weight=down_weight, attention_gain=attention_gain, feedforward_gain=feedforward_gain, encoded=encoded, send_rows=send_rows, send_count=send_count, arrival_nodes=arrival_nodes, sage_weight=sage_weight, node_gain=node_gain)


LN_EPSILON = 1e-12

def layer_norm(values, gain):
    center = values - lax.optimization_barrier(jnp.mean(values, axis=-1, keepdims=True))
    spread = lax.optimization_barrier(jnp.mean(center * center, axis=-1, keepdims=True))
    return center * lax.rsqrt(spread + LN_EPSILON) * gain

def encode_titles(states, tokens, query_key_value, output_weight, up_weight, down_weight, attention_gain, feedforward_gain):
    titles = states.shape[0]
    flat = states.reshape(titles * SEQ, D)
    live = tokens != 0
    projected = jnp.dot(flat, query_key_value, preferred_element_type=jnp.float32).astype(jnp.bfloat16)
    projected = lax.optimization_barrier(projected)
    projected = projected.reshape(titles, SEQ, 3, HEADS, HEAD_DIM).astype(jnp.float32)
    query_states = projected[:, :, 0]
    key_states = projected[:, :, 1]
    value_states = projected[:, :, 2]
    scores = jnp.einsum('tihd,tjhd->thij', query_states, key_states) * (1.0 / math.sqrt(HEAD_DIM))
    scores = jnp.where(live[:, None, None, :], scores, -jnp.inf)
    highest = lax.optimization_barrier(jnp.max(scores, axis=-1, keepdims=True))
    weights = jnp.exp(scores - highest)
    probs = (weights / lax.optimization_barrier(jnp.sum(weights, axis=-1, keepdims=True))).astype(jnp.bfloat16)
    probs = lax.optimization_barrier(probs)
    context = jnp.einsum('thij,tjhd->tihd', probs.astype(jnp.float32), value_states)
    context = context.astype(jnp.bfloat16).reshape(titles * SEQ, D)
    mixed = jnp.dot(context, output_weight, preferred_element_type=jnp.float32)
    attended = layer_norm(flat.astype(jnp.float32) + mixed, attention_gain).astype(jnp.bfloat16)
    attended = lax.optimization_barrier(attended)
    inner = jax.nn.gelu(jnp.dot(attended, up_weight, preferred_element_type=jnp.float32), approximate=False)
    inner = inner.astype(jnp.bfloat16)
    lowered = jnp.dot(inner, down_weight, preferred_element_type=jnp.float32)
    token_out = layer_norm(attended.astype(jnp.float32) + lowered, feedforward_gain).reshape(titles, SEQ, D)
    live_weight = live.astype(jnp.float32)
    pooled = lax.optimization_barrier(jnp.sum(token_out * live_weight[:, :, None], axis=1)) / lax.optimization_barrier(jnp.sum(live_weight, axis=1, keepdims=True))
    return pooled.astype(jnp.bfloat16)

def reference(hidden_states, title_tokens, query_key_value, output_weight, up_weight, down_weight, attention_gain, feedforward_gain, encoded, send_rows, send_count, arrival_nodes, sage_weight, node_gain):

    def one_device(element):
        return encode_titles(element[0], element[1], query_key_value, output_weight, up_weight, down_weight, attention_gain, feedforward_gain)
    pooled = lax.map(one_device, (hidden_states.reshape(DEVICES, TITLES_DEV, SEQ, D), title_tokens.reshape(DEVICES, TITLES_DEV, SEQ)))
    title_vectors = pooled.reshape(TITLES, D)
    sources = jnp.arange(DEVICES, dtype=jnp.int32)
    slots = jnp.arange(CAP, dtype=jnp.int32)

    def one_receiver(element):
        rows_from, counts_from, targets = element
        index = (sources[:, None] * NODES_DEV + rows_from).reshape(-1).astype(jnp.int32)
        rows = jnp.take(encoded, index, axis=0).astype(jnp.float32)
        valid = (slots[None, :] < counts_from[:, None]).reshape(-1).astype(jnp.float32)
        labels = targets.reshape(-1).astype(jnp.int32)
        sums = jax.ops.segment_sum(rows * valid[:, None], labels, num_segments=NODES_DEV)
        degree = jax.ops.segment_sum(valid, labels, num_segments=NODES_DEV)
        return (sums / jnp.maximum(degree, 1.0)[:, None]).astype(jnp.bfloat16)
    neighbour_mean = lax.map(one_receiver, (jnp.transpose(send_rows, (1, 0, 2)), jnp.transpose(send_count), arrival_nodes))
    neighbour_mean = neighbour_mean.reshape(NODES, D)
    own_rows = encoded.reshape(DEVICES, NODES_DEV, D)
    self_rows = jnp.concatenate([pooled, own_rows[:, TITLES_DEV:]], axis=1).reshape(NODES, D)
    combined = jnp.dot(self_rows, sage_weight[0], preferred_element_type=jnp.float32)
    combined = combined + jnp.dot(neighbour_mean, sage_weight[1], preferred_element_type=jnp.float32)
    node_output = layer_norm(combined, node_gain).astype(jnp.bfloat16)
    return (title_vectors, node_output)
```

```python
import functools
import math

import jax
import jax.numpy as jnp
from jax import lax
from jax.experimental import pallas as pl
from jax.experimental.pallas import tpu as pltpu
from jax.sharding import PartitionSpec as P

MESH = pl.DeviceIdType.MESH

HEADS = 12
HEAD_DIM = 64


LN_EPSILON = 1e-12


def layer_norm(values, gain):
    center = values - jnp.mean(values, axis=-1, keepdims=True)
    spread = jnp.mean(center * center, axis=-1, keepdims=True)
    return center * lax.rsqrt(spread + LN_EPSILON) * gain


def gather_kernel(outer, inner, arity, *refs):
    shards, fulls = refs[:arity], refs[arity : 2 * arity]
    (own_sem, outer_send, outer_recv, inner_send, inner_recv, pair_send, pair_recv, core_send, core_recv) = refs[2 * arity :]
    me = lax.axis_index("fsdp")
    spot = lax.axis_index("dom")
    row, column = me // inner, lax.rem(me, inner)
    base = (spot // 4) * 4
    side = lax.rem(spot, 4) // 2
    core = lax.rem(spot, 2)
    pair_peer = base + (1 - side) * 2 + core
    core_peer = base + side * 2 + (1 - core)
    outer_peers = [lax.rem(row + step, outer) * inner + column for step in range(1, outer)]
    inner_peers = [row * inner + lax.rem(column + step, inner) for step in range(1, inner)]

    barrier = pltpu.get_barrier_semaphore()
    for peer in outer_peers + inner_peers:
        pl.semaphore_signal(barrier, inc=1, device_id=(peer, spot), device_id_type=MESH)
    for peer in (pair_peer, core_peer):
        pl.semaphore_signal(barrier, inc=1, device_id=(me, peer), device_id_type=MESH)
    pl.semaphore_wait(barrier, outer + inner)

    def part(ref, start, count):
        if len(ref.shape) == 3:
            return ref.at[:, pl.ds(start, count), :]
        return ref.at[pl.ds(start, count), :]

    def rows_of(which):
        return shards[which].shape[-2]

    def unit_of(which):
        return rows_of(which) // 6

    def block_start(which, back, over):
        owner = lax.rem(row - back + outer, outer) * inner + lax.rem(column - over + inner, inner)
        return pl.multiple_of(owner * rows_of(which), 8)

    def own_copy(which):
        return pltpu.make_async_copy(
            shards[which],
            part(fulls[which], block_start(which, 0, 0), rows_of(which)),
            own_sem.at[which],
        )

    def outer_copy(which, step, receive=False):
        unit = unit_of(which)
        first = (3 * core + side) * unit
        back = step if receive else 0
        return pltpu.make_async_remote_copy(
            src_ref=part(shards[which], pl.multiple_of(first, 8), 2 * unit),
            dst_ref=part(fulls[which], pl.multiple_of(block_start(which, back, 0) + first, 8), 2 * unit),
            send_sem=outer_send.at[which, step - 1],
            recv_sem=outer_recv.at[which, step - 1],
            device_id=(outer_peers[step - 1], spot),
            device_id_type=MESH,
        )

    def inner_copy(which, back, over, receive=False):
        unit = unit_of(which)
        first = (3 * core + side) * unit
        target = part(
            fulls[which],
            pl.multiple_of(block_start(which, back, over if receive else 0) + first, 8),
            2 * unit,
        )
        if back == 0 and not receive:
            source = part(shards[which], pl.multiple_of(first, 8), 2 * unit)
        else:
            source = target
        return pltpu.make_async_remote_copy(
            src_ref=source,
            dst_ref=target,
            send_sem=inner_send.at[which, back, over - 1],
            recv_sem=inner_recv.at[which, back, over - 1],
            device_id=(inner_peers[over - 1], spot),
            device_id_type=MESH,
        )

    def pair_copy(which, back, over, receive=False):
        unit = unit_of(which)
        edge = 1 - side if receive else side
        piece = part(
            fulls[which],
            pl.multiple_of(block_start(which, back, over) + (3 * core + 2 * edge) * unit, 8),
            unit,
        )
        return pltpu.make_async_remote_copy(
            src_ref=piece,
            dst_ref=piece,
            send_sem=pair_send.at[which, back, over],
            recv_sem=pair_recv.at[which, back, over],
            device_id=(me, pair_peer),
            device_id_type=MESH,
        )

    def core_copy(which, back, over, receive=False):
        unit = unit_of(which)
        half = 1 - core if receive else core
        piece = part(
            fulls[which],
            pl.multiple_of(block_start(which, back, over) + 3 * half * unit, 8),
            3 * unit,
        )
        return pltpu.make_async_remote_copy(
            src_ref=piece,
            dst_ref=piece,
            send_sem=core_send.at[which, back, over],
            recv_sem=core_recv.at[which, back, over],
            device_id=(me, core_peer),
            device_id_type=MESH,
        )

    blocks = [(back, over) for over in range(inner) for back in range(outer) if (back, over) != (0, 0)]

    for which in range(arity):
        for step in range(outer - 1, 0, -1):
            outer_copy(which, step).start()
        for over in range(1, inner):
            inner_copy(which, 0, over).start()
        own_copy(which).start()

    def outer_stage(which):
        for step in range(1, outer):
            outer_copy(which, step, receive=True).wait_recv()
            for over in range(1, inner):
                inner_copy(which, step, over).start()
            pair_copy(which, step, 0).start()

    def inner_stage(which):
        for over in range(1, inner):
            for back in range(outer):
                inner_copy(which, back, over, receive=True).wait_recv()
                pair_copy(which, back, over).start()

    def pair_stage(which):
        for back, over in blocks:
            pair_copy(which, back, over, receive=True).wait_recv()
            core_copy(which, back, over).start()

    for tick in range(arity + 2):
        if tick < arity:
            outer_stage(tick)
        if 0 <= tick - 1 < arity:
            inner_stage(tick - 1)
        if 0 <= tick - 2 < arity:
            pair_stage(tick - 2)

    for which in range(arity):
        own_copy(which).wait()
        for step in range(1, outer):
            outer_copy(which, step).wait_send()
        for over in range(1, inner):
            for back in range(outer):
                inner_copy(which, back, over).wait_send()
        for back, over in blocks:
            pair_copy(which, back, over).wait_send()
            core_copy(which, back, over).wait_send()
            core_copy(which, back, over, receive=True).wait_recv()


def gather_weights(fsdp, *weights):
    outer = 4 if fsdp % 4 == 0 else 1
    inner = fsdp // outer
    arity = len(weights)
    shapes = []
    for weight in weights:
        shape = list(weight.shape)
        shape[-2] *= fsdp
        shapes.append(jax.ShapeDtypeStruct(tuple(shape), weight.dtype))
    dma = pltpu.SemaphoreType.DMA
    moved = sum(weight.size * weight.dtype.itemsize for weight in weights)
    return pl.pallas_call(
        functools.partial(gather_kernel, outer, inner, arity),
        out_shape=tuple(shapes),
        in_specs=[pl.BlockSpec(memory_space=pltpu.VMEM)] * arity,
        out_specs=tuple([pl.BlockSpec(memory_space=pl.ANY)] * arity),
        scratch_shapes=[
            dma((arity,)),
            dma((arity, outer - 1)),
            dma((arity, outer - 1)),
            dma((arity, outer, inner - 1)),
            dma((arity, outer, inner - 1)),
            dma((arity, outer, inner)),
            dma((arity, outer, inner)),
            dma((arity, outer, inner)),
            dma((arity, outer, inner)),
        ],
        compiler_params=pltpu.CompilerParams(collective_id=0, has_side_effects=True),
        cost_estimate=pl.CostEstimate(flops=60_000_000_000, bytes_accessed=moved * fsdp, transcendentals=0),
        name="gather_weights",
    )(*weights)


def encode_titles(
    hidden_states,
    title_tokens,
    full_project,
    full_output,
    full_up,
    full_down,
    attention_gain,
    feedforward_gain,
):
    titles, seq_len, width = hidden_states.shape
    flat = hidden_states.reshape(titles * seq_len, width)
    live = title_tokens != 0
    projected = jnp.dot(flat, full_project, preferred_element_type=jnp.float32).astype(jnp.bfloat16)
    projected = projected.reshape(titles, seq_len, 3, HEADS, HEAD_DIM)
    query_states = projected[:, :, 0]
    key_states = projected[:, :, 1]
    value_states = projected[:, :, 2]
    scores = jnp.einsum(
        "tihd,tjhd->thij", query_states, key_states, preferred_element_type=jnp.float32
    )
    scores = scores * (1.0 / math.sqrt(HEAD_DIM))
    scores = jnp.where(live[:, None, None, :], scores, -jnp.inf)
    highest = jnp.max(scores, axis=-1, keepdims=True)
    weights = jnp.exp(scores - highest)
    probs = (weights / jnp.sum(weights, axis=-1, keepdims=True)).astype(jnp.bfloat16)
    context = jnp.einsum("thij,tjhd->tihd", probs, value_states, preferred_element_type=jnp.float32)
    context = context.astype(jnp.bfloat16).reshape(titles * seq_len, width)
    mixed = jnp.dot(context, full_output, preferred_element_type=jnp.float32)
    attended = layer_norm(flat.astype(jnp.float32) + mixed, attention_gain).astype(jnp.bfloat16)
    attended = lax.optimization_barrier(attended)
    inner = jax.nn.gelu(
        jnp.dot(attended, full_up, preferred_element_type=jnp.float32), approximate=False
    )
    inner = inner.astype(jnp.bfloat16)
    lowered = jnp.dot(inner, full_down, preferred_element_type=jnp.float32)
    token_out = layer_norm(attended.astype(jnp.float32) + lowered, feedforward_gain).reshape(
        titles, seq_len, width
    )
    live_weight = live.astype(jnp.float32)
    pooled = jnp.sum(token_out * live_weight[:, :, None], axis=1) / jnp.sum(
        live_weight, axis=1, keepdims=True
    )
    return pooled.astype(jnp.bfloat16)


def scatter_sums(arrived, targets, valid, nodes):
    width = arrived.shape[2]
    mask_flat = valid.reshape(-1).astype(jnp.float32)
    label_flat = targets.reshape(-1)
    rows = arrived.reshape(-1, width).astype(jnp.float32) * mask_flat[:, None]
    sums = jax.ops.segment_sum(rows, label_flat, num_segments=nodes)
    degree = jax.ops.segment_sum(mask_flat, label_flat, num_segments=nodes)
    return (sums, degree)


def on_device(
    fsdp,
    hidden_states,
    title_tokens,
    query_key_value,
    output_weight,
    up_weight,
    down_weight,
    attention_gain,
    feedforward_gain,
    encoded,
    send_rows,
    send_count,
    arrival_nodes,
    sage_weight,
    node_gain,
):
    titles = hidden_states.shape[0]
    nodes, width = encoded.shape
    outgoing = jnp.take(encoded, send_rows[0], axis=0)
    slot_count = outgoing.shape[1]
    counts_out = send_count[0].astype(jnp.bfloat16)
    arrived, arrived_counts = (
        lax.all_to_all(outgoing, ("fsdp", "dom"), split_axis=0, concat_axis=0, tiled=True),
        lax.all_to_all(counts_out, ("fsdp", "dom"), split_axis=0, concat_axis=0, tiled=True),
    )
    valid = (
        jnp.arange(slot_count, dtype=jnp.int32)[None, :] < arrived_counts.astype(jnp.int32)[:, None]
    )
    targets = arrival_nodes[0]
    full_project, full_output, full_up, full_down, piece = gather_weights(
        fsdp, query_key_value, output_weight, up_weight, down_weight, sage_weight
    )
    title_vectors = encode_titles(
        hidden_states,
        title_tokens,
        full_project,
        full_output,
        full_up,
        full_down,
        attention_gain,
        feedforward_gain,
    )
    sums, degree = scatter_sums(arrived, targets, valid, nodes)
    neighbour_mean = (sums / jnp.maximum(degree, 1.0)[:, None]).astype(jnp.bfloat16)
    self_rows = jnp.concatenate([title_vectors, encoded[titles:]], axis=0)
    running = jnp.dot(self_rows, piece[0], preferred_element_type=jnp.float32)
    combined = running + jnp.dot(neighbour_mean, piece[1], preferred_element_type=jnp.float32)
    node_output = layer_norm(combined, node_gain).astype(jnp.bfloat16)
    return (title_vectors, node_output)


def solution(mesh):
    return jax.shard_map(
        functools.partial(on_device, mesh.shape["fsdp"]),
        mesh=mesh,
        in_specs=(
            P(("fsdp", "dom"), None, None),
            P(("fsdp", "dom"), None),
            P("fsdp", None),
            P("fsdp", None),
            P("fsdp", None),
            P("fsdp", None),
            P(),
            P(),
            P(("fsdp", "dom"), None),
            P(("fsdp", "dom"), None, None),
            P(("fsdp", "dom"), None),
            P(("fsdp", "dom"), None, None),
            P(None, "fsdp", None),
            P(),
        ),
        out_specs=(P(("fsdp", "dom"), None), P(("fsdp", "dom"), None)),
        check_vma=False,
    )
```
